32 devices in a mesh: dp: 4 (over y, z), ep: 8 (over x, core).
Axes of the slice: x: 4, y: 2, z: 2, core: 2. Of those that a mesh axis runs over, the one named last changes fastest.
The devices are a block of a 4x4x8 slice.
Arguments:
- tokens: bfloat16 [2, 64, 256, 1536], P(None, ('dp', 'ep')), parts along dimension 1
- expert_ids: int32 [2, 16384, 6], P(None, ('dp', 'ep')), parts along dimension 1
- route_weights: float32 [2, 16384, 6], P(None, ('dp', 'ep')), parts along dimension 1
- attn_norm: bfloat16 [1536], replicated
- w_query: bfloat16 [1536, 12, 128], replicated
- w_key: bfloat16 [1536, 12, 128], replicated
- w_value: bfloat16 [1536, 12, 128], replicated
- w_out: bfloat16 [12, 128, 1536], replicated
- ffn_norm: bfloat16 [1536], replicated
- w_gate: bfloat16 [64, 1536, 512], P('ep')
- w_up: bfloat16 [64, 1536, 512], P('ep')
- w_down: bfloat16 [64, 512, 1536], P('ep')
- shared_gate: bfloat16 [1536, 1024], replicated
- shared_up: bfloat16 [1536, 1024], replicated
- shared_down: bfloat16 [1024, 1536], replicated
Outputs:
- output: bfloat16 [2, 64, 256, 1536], P(None, ('dp', 'ep')), parts along dimension 1
There are 4 independent parts. The reference program is written for one: setup_inputs(seed, part) draws one part's arguments, and reference() takes and returns one part's arrays. A program takes and returns all parts, laid end to end along the dimension named above; an argument that names none is the same for every part.
All inputs are finite; a program needn't handle non-finite values.
Results may differ from the reference program's by a relative error of at most 0.0102355.
Values are sent between devices in bfloat16 or wider.
A program may use at most 768 MiB of HBM per device.

```python
import jax
import jax.numpy as jnp
import numpy as np
from jax import lax

TOKENS = 512
SEQ = 256
D_MODEL = 1536
HEADS = 12
HEAD_DIM = 128
EXPERTS = 64
TOP = 6
FF = 512
SHARED_FF = 1024
GROUP = 8
CAPACITY = 96
NORM_EPS = 1e-6


def load_profile():
    total_rows = TOKENS * TOP
    rest_rows = total_rows - CAPACITY
    weight_list = [3 * (EXPERTS - 1) - 2 * rank_pos for rank_pos in range(EXPERTS - 1)]
    weight_sum = sum(weight_list)
    count_list = [rest_rows * weight_val // weight_sum for weight_val in weight_list]
    extra_units = rest_rows - sum(count_list)
    count_list = [count_val + (1 if rank_pos < extra_units else 0) for rank_pos, count_val in enumerate(count_list)]
    return [CAPACITY] + count_list


def draw_routing(base_key):
    rank_ids = np.repeat(np.arange(EXPERTS), np.array(load_profile()))

    def one_micro(micro_key):
        sub_keys = jax.random.split(micro_key)
        expert_of_rank = jax.random.permutation(sub_keys[0], EXPERTS)
        id_grid = expert_of_rank[rank_ids].reshape(TOP, TOKENS).T
        device_keys = jax.random.split(sub_keys[1], GROUP)

        def one_device(device_key):
            return id_grid[jax.random.permutation(device_key, TOKENS)]

        return jax.vmap(one_device)(device_keys).reshape(GROUP * TOKENS, TOP)

    return jax.vmap(one_micro)(jax.random.split(base_key, 2)).astype(jnp.int32)


def draw_normal(sub_key, array_shape, std_scale):
    return (jax.random.normal(sub_key, array_shape, jnp.float32) * std_scale).astype(jnp.bfloat16)


def setup_inputs(seed: int = 0, part: int = 0) -> dict:
    weight_keys = jax.random.split(jax.random.key(seed), 12)
    part_keys = jax.random.split(jax.random.fold_in(jax.random.key(seed + 1), part), 3)
    n_rows = GROUP * TOKENS
    attn_width = HEADS * HEAD_DIM
    return {
        "tokens": draw_normal(part_keys[0], (2, n_rows // SEQ, SEQ, D_MODEL), 1.0),
        "expert_ids": draw_routing(part_keys[1]),
        "route_weights": jax.nn.softmax(jax.random.normal(part_keys[2], (2, n_rows, TOP), jnp.float32), axis=-1),
        "attn_norm": jax.random.uniform(weight_keys[0], (D_MODEL,), jnp.float32, 0.5, 1.5).astype(jnp.bfloat16),
        "w_query": draw_normal(weight_keys[1], (D_MODEL, HEADS, HEAD_DIM), D_MODEL ** -0.5),
        "w_key": draw_normal(weight_keys[2], (D_MODEL, HEADS, HEAD_DIM), D_MODEL ** -0.5),
        "w_value": draw_normal(weight_keys[3], (D_MODEL, HEADS, HEAD_DIM), D_MODEL ** -0.5),
        "w_out": draw_normal(weight_keys[4], (HEADS, HEAD_DIM, D_MODEL), attn_width ** -0.5),
        "ffn_norm": jax.random.uniform(weight_keys[5], (D_MODEL,), jnp.float32, 0.5, 1.5).astype(jnp.bfloat16),
        "w_gate": draw_normal(weight_keys[6], (EXPERTS, D_MODEL, FF), D_MODEL ** -0.5),
        "w_up": draw_normal(weight_keys[7], (EXPERTS, D_MODEL, FF), D_MODEL ** -0.5),
        "w_down": draw_normal(weight_keys[8], (EXPERTS, FF, D_MODEL), 2.0 * FF ** -0.5),
        "shared_gate": draw_normal(weight_keys[9], (D_MODEL, SHARED_FF), D_MODEL ** -0.5),
        "shared_up": draw_normal(weight_keys[10], (D_MODEL, SHARED_FF), D_MODEL ** -0.5),
        "shared_down": draw_normal(weight_keys[11], (SHARED_FF, D_MODEL), SHARED_FF ** -0.5),
    }


def rms_norm(in_vals, norm_gain):
    wide_vals = in_vals.astype(jnp.float32)
    inv_rms = lax.rsqrt(jnp.mean(wide_vals * wide_vals, axis=-1, keepdims=True) + NORM_EPS)
    return (wide_vals * inv_rms * norm_gain.astype(jnp.float32)).astype(jnp.bfloat16)


def attention_block(seq_rows, attn_norm, w_query, w_key, w_value, w_out):
    n_seq = seq_rows.shape[0]
    normed = rms_norm(seq_rows, attn_norm).reshape(n_seq * SEQ, D_MODEL)

    def project(weight):
        proj_rows = jnp.dot(normed, weight.reshape(D_MODEL, HEADS * HEAD_DIM), preferred_element_type=jnp.float32)
        return proj_rows.astype(jnp.bfloat16).reshape(n_seq, SEQ, HEADS, HEAD_DIM)

    queries = project(w_query)
    key_rows = project(w_key)
    value_rows = project(w_value)
    scores = jnp.einsum("bqhe,bkhe->bhqk", queries.astype(jnp.float32), key_rows.astype(jnp.float32)) * HEAD_DIM ** -0.5
    causal = jnp.arange(SEQ)[:, None] >= jnp.arange(SEQ)[None, :]
    attn_probs = jax.nn.softmax(jnp.where(causal, scores, -jnp.inf), axis=-1).astype(jnp.bfloat16)
    head_mix = jnp.einsum("bhqk,bkhe->bqhe", attn_probs.astype(jnp.float32), value_rows.astype(jnp.float32)).astype(jnp.bfloat16)
    attn_out = jnp.dot(head_mix.reshape(n_seq * SEQ, HEADS * HEAD_DIM), w_out.reshape(HEADS * HEAD_DIM, D_MODEL), preferred_element_type=jnp.float32)
    return (seq_rows.astype(jnp.float32) + attn_out.reshape(n_seq, SEQ, D_MODEL)).astype(jnp.bfloat16)


def swiglu(in_rows, gate_w, up_w, down_w):
    gate_act = jnp.dot(in_rows, gate_w, preferred_element_type=jnp.float32)
    up_act = jnp.dot(in_rows, up_w, preferred_element_type=jnp.float32)
    hidden = (jax.nn.silu(gate_act) * up_act).astype(jnp.bfloat16)
    return jnp.dot(hidden, down_w, preferred_element_type=jnp.float32).astype(jnp.bfloat16)


def route_plan(flat_ids, slot_cap):
    n_rows = flat_ids.shape[0]
    sort_order = jnp.argsort(flat_ids, stable=True).astype(jnp.int32)
    counts = jnp.bincount(flat_ids, length=EXPERTS)
    starts = jnp.cumsum(counts) - counts
    sorted_rank = jnp.zeros((n_rows,), jnp.int32).at[sort_order].set(jnp.arange(n_rows, dtype=jnp.int32))
    slot_ids = sorted_rank - starts[flat_ids]
    src_pos = sort_order[jnp.minimum(starts[:, None] + jnp.arange(slot_cap)[None, :], n_rows - 1)]
    return slot_ids, src_pos


def reference(tokens, expert_ids, route_weights, attn_norm, w_query, w_key, w_value, w_out, ffn_norm, w_gate, w_up, w_down, shared_gate, shared_up, shared_down):
    def one_micro(micro_inputs):
        micro_tok, micro_ids, micro_weights = micro_inputs
        dev_seqs = micro_tok.reshape(GROUP, TOKENS // SEQ, SEQ, D_MODEL)
        residual = lax.map(lambda dev_rows: attention_block(dev_rows, attn_norm, w_query, w_key, w_value, w_out), dev_seqs)
        residual = residual.reshape(GROUP * TOKENS, D_MODEL)
        normed = rms_norm(residual, ffn_norm)
        shared_out = swiglu(normed, shared_gate, shared_up, shared_down)
        flat_ids = micro_ids.reshape(-1)
        slot_cap = GROUP * CAPACITY
        slot_ids, src_pos = route_plan(flat_ids, slot_cap)
        expert_in = normed[src_pos // TOP]
        expert_out = lax.map(lambda packed: swiglu(packed[0], packed[1], packed[2], packed[3]), (expert_in, w_gate, w_up, w_down))
        picked = expert_out.reshape(EXPERTS * slot_cap, D_MODEL)[flat_ids * slot_cap + slot_ids]
        picked = picked.reshape(GROUP * TOKENS, TOP, D_MODEL)
        routed = jnp.sum(picked.astype(jnp.float32) * micro_weights[:, :, None], axis=1)
        layer_rows = residual.astype(jnp.float32) + shared_out.astype(jnp.float32) + routed
        return layer_rows.astype(jnp.bfloat16).reshape(micro_tok.shape)

    return lax.map(one_micro, (tokens, expert_ids, route_weights))
```

```python
import functools

import jax
import jax.numpy as jnp
from jax import lax
from jax.experimental import pallas as pl
from jax.experimental.pallas import tpu as pltpu
from jax.sharding import PartitionSpec as P


NORM_EPS = 1e-6
CAP_FACTOR = 2
SLOT_ALIGN = 8
CORES = 2
WEIGHTS_AHEAD = 2


def capacity_of(n_tok, top_count, experts):
    return SLOT_ALIGN * ((CAP_FACTOR * n_tok * top_count + SLOT_ALIGN * experts - 1) // (SLOT_ALIGN * experts))


def rms_norm(in_vals, norm_gain):
    wide_vals = in_vals.astype(jnp.float32)
    inv_rms = lax.rsqrt(jnp.mean(wide_vals * wide_vals, axis=-1, keepdims=True) + NORM_EPS)
    return (wide_vals * inv_rms * norm_gain.astype(jnp.float32)).astype(jnp.bfloat16)


def attention_block(seq_rows, attn_norm, w_query, w_key, w_value, w_out):
    normed = rms_norm(seq_rows, attn_norm)
    queries = jnp.einsum("...sd,dhe->...she", normed, w_query, preferred_element_type=jnp.float32).astype(jnp.bfloat16)
    key_rows = jnp.einsum("...sd,dhe->...she", normed, w_key, preferred_element_type=jnp.float32).astype(jnp.bfloat16)
    value_rows = jnp.einsum("...sd,dhe->...she", normed, w_value, preferred_element_type=jnp.float32).astype(jnp.bfloat16)
    seq_len = seq_rows.shape[-2]
    scores = jnp.einsum("...qhe,...khe->...hqk", queries, key_rows, preferred_element_type=jnp.float32) * (w_query.shape[-1] ** -0.5)
    causal = jnp.arange(seq_len)[:, None] >= jnp.arange(seq_len)[None, :]
    attn_probs = jax.nn.softmax(jnp.where(causal, scores, -jnp.inf), axis=-1).astype(jnp.bfloat16)
    head_mix = jnp.einsum("...hqk,...khe->...qhe", attn_probs, value_rows, preferred_element_type=jnp.float32).astype(jnp.bfloat16)
    attn_out = jnp.einsum("...qhe,hed->...qd", head_mix, w_out, preferred_element_type=jnp.float32)
    return (seq_rows.astype(jnp.float32) + attn_out).astype(jnp.bfloat16)


def swiglu(in_rows, gate_w, up_w, down_w):
    gate_act = jnp.dot(in_rows, gate_w, preferred_element_type=jnp.float32)
    up_act = jnp.dot(in_rows, up_w, preferred_element_type=jnp.float32)
    hidden = (jax.nn.silu(gate_act) * up_act).astype(jnp.bfloat16)
    return jnp.dot(hidden, down_w, preferred_element_type=jnp.float32).astype(jnp.bfloat16)


def expert_kernel(parts, adds, n_src, n_piece, cap, rank_ref, wt_ref, *refs):
    pieces = refs[:n_piece]
    gate_hbm, up_hbm, down_hbm = refs[n_piece : n_piece + 3]
    outs = refs[n_piece + 3 : n_piece + 3 + n_src]
    z_buf, g_buf, u_buf, w_buf, d_buf, c_buf, x_buf, o_buf, z_sem, w_sem, o_sem, q_sem = refs[n_piece + 3 + n_src :]
    n_exp = g_buf.shape[0]
    n_tok = z_buf.shape[1]

    z_copies = [
        [
            pltpu.make_async_copy(pieces[p], z_buf.at[src, pl.ds(row, rows), :], z_sem.at[src, k])
            for k, (p, row, rows) in enumerate(parts[src])
        ]
        for src in range(n_src)
    ]
    for src in range(n_src):
        for c in z_copies[src]:
            c.start()

    def w_copies(e):
        return [
            pltpu.make_async_copy(h.at[e], b.at[e], w_sem.at[k, e])
            for k, (h, b) in enumerate(((gate_hbm, g_buf), (up_hbm, u_buf), (down_hbm, w_buf)))
        ]

    for e in range(WEIGHTS_AHEAD):
        for c in w_copies(e):
            c.start()
    q_copies = [
        None if adds[src] is None else pltpu.make_async_copy(pieces[adds[src]], o_buf.at[src], q_sem.at[src])
        for src in range(n_src)
    ]

    slot_iota = lax.broadcasted_iota(jnp.int32, (cap, n_tok), 0).astype(jnp.float32)
    for src in range(n_src):
        for e in range(n_exp):
            hit = slot_iota == rank_ref[src, e : e + 1, :]
            d_buf[e * cap : (e + 1) * cap, :] = jnp.where(hit, 1.0, 0.0).astype(jnp.bfloat16)
        for c in z_copies[src]:
            c.wait()
        picked = jnp.dot(d_buf[...], z_buf[src], preferred_element_type=jnp.float32).astype(jnp.bfloat16)
        for e in range(n_exp):
            x_buf[e, src * cap : (src + 1) * cap, :] = picked[e * cap : (e + 1) * cap, :]

    def ffn(e, carry):
        @pl.when(e + WEIGHTS_AHEAD < n_exp)
        def _():
            for c in w_copies(e + WEIGHTS_AHEAD):
                c.start()

        for c in w_copies(e):
            c.wait()
        rows = x_buf[e]
        gate = jnp.dot(rows, g_buf[e], preferred_element_type=jnp.float32)
        up = jnp.dot(rows, u_buf[e], preferred_element_type=jnp.float32)
        hidden = (gate * jax.nn.sigmoid(gate) * up).astype(jnp.bfloat16)
        x_buf[e] = jnp.dot(hidden, w_buf[e], preferred_element_type=jnp.float32).astype(jnp.bfloat16)
        return carry

    lax.fori_loop(0, n_exp - 1, ffn, 0)
    for c in q_copies:
        if c is not None:
            c.start()
    ffn(n_exp - 1, 0)

    out_copies = [pltpu.make_async_copy(o_buf.at[src], outs[src], o_sem.at[src]) for src in range(n_src)]
    for src in range(n_src):
        for e in range(n_exp):
            hit = slot_iota == rank_ref[src, e : e + 1, :]
            w0 = wt_ref[src, e : e + 1, :]
            hi = w0.astype(jnp.bfloat16).astype(jnp.float32)
            w1 = w0 - hi
            mid = w1.astype(jnp.bfloat16).astype(jnp.float32)
            for t, term in enumerate((hi, mid, w1 - mid)):
                c_buf[t, e * cap : (e + 1) * cap, :] = jnp.where(hit, term, 0.0).astype(jnp.bfloat16)
        rows = jnp.concatenate([x_buf[e, src * cap : (src + 1) * cap, :] for e in range(n_exp)], axis=0)
        acc = None
        for t in range(3):
            term = lax.dot_general(c_buf[t], rows, (((0,), (0,)), ((), ())), preferred_element_type=jnp.float32)
            acc = term if acc is None else acc + term
        if q_copies[src] is None:
            o_buf[src] = acc
        else:
            q_copies[src].wait()
            o_buf[src] = o_buf[src] + acc
        out_copies[src].start()
    for c in out_copies:
        c.wait()


def expert_call(sources, adds, rank, wts, w_gate, w_up, w_down, cap):
    n_src = len(sources)
    n_exp, d_model, d_ff = w_gate.shape
    n_tok = rank.shape[-1]
    pieces, parts, add_at = [], [], []
    for src in sources:
        row, lst = 0, []
        for piece in src:
            lst.append((len(pieces), row, piece.shape[0]))
            pieces.append(piece)
            row += piece.shape[0]
        parts.append(lst)
    for add in adds:
        add_at.append(None if add is None else len(pieces))
        if add is not None:
            pieces.append(add)
    max_parts = max(len(p) for p in parts)
    flops = 2 * n_src * n_exp * cap * (3 * d_model * d_ff + 4 * n_tok * d_model)
    hbm = pl.BlockSpec(memory_space=pl.ANY)
    vmem = pl.BlockSpec(memory_space=pltpu.VMEM)
    return pl.pallas_call(
        functools.partial(expert_kernel, parts, add_at, n_src, len(pieces), cap),
        out_shape=[jax.ShapeDtypeStruct((n_tok, d_model), jnp.float32)] * n_src,
        in_specs=[vmem, vmem] + [hbm] * (len(pieces) + 3),
        out_specs=[hbm] * n_src,
        scratch_shapes=[
            pltpu.VMEM((n_src, n_tok, d_model), jnp.bfloat16),
            pltpu.VMEM((n_exp, d_model, d_ff), jnp.bfloat16),
            pltpu.VMEM((n_exp, d_model, d_ff), jnp.bfloat16),
            pltpu.VMEM((n_exp, d_ff, d_model), jnp.bfloat16),
            pltpu.VMEM((n_exp * cap, n_tok), jnp.bfloat16),
            pltpu.VMEM((3, n_exp * cap, n_tok), jnp.bfloat16),
            pltpu.VMEM((n_exp, n_src * cap, d_model), jnp.bfloat16),
            pltpu.VMEM((n_src, n_tok, d_model), jnp.float32),
            pltpu.SemaphoreType.DMA((n_src, max_parts)),
            pltpu.SemaphoreType.DMA((3, n_exp)),
            pltpu.SemaphoreType.DMA((n_src,)),
            pltpu.SemaphoreType.DMA((n_src,)),
        ],
        compiler_params=pltpu.CompilerParams(vmem_limit_bytes=65_400_000),
        cost_estimate=pl.CostEstimate(flops=flops, bytes_accessed=60_000_000, transcendentals=0),
        name="experts",
    )(rank, wts, *pieces, w_gate, w_up, w_down)


def solution(mesh):
    group_size = mesh.shape["ep"]
    chips = group_size // CORES

    def shift(x, d_chip, d_core=0):
        pairs = [
            (i, (((i // CORES + d_chip) % chips) * CORES + i % CORES) ^ d_core)
            for i in range(group_size)
        ]
        return lax.ppermute(x, "ep", pairs)

    def twin(x):
        return shift(x, 0, 1)

    def device_step(tokens, expert_ids, route_weights, attn_norm, w_query, w_key, w_value, w_out, ffn_norm, w_gate, w_up, w_down, shared_gate, shared_up, shared_down):
        n_micro, n_seq, seq_len, d_model = tokens.shape
        n_tok = n_seq * seq_len
        half = n_tok // 2
        top_count = expert_ids.shape[-1]
        local_experts = w_gate.shape[0]
        experts = local_experts * group_size
        cap = capacity_of(n_tok, top_count, experts)

        info = jnp.concatenate(
            [expert_ids.astype(jnp.float32).transpose(0, 2, 1), route_weights.transpose(0, 2, 1)], axis=1
        )
        rel = [(2, 0), (2, 1), (1, 0), (1, 1), (3, 0), (3, 1), (0, 0), (0, 1)]
        infos = jnp.stack([info if r == (0, 0) else shift(info, *r) for r in rel], axis=1)
        ids = infos[:, :, :top_count]
        wts = infos[:, :, top_count:]
        base = (lax.axis_index("ep") * local_experts).astype(jnp.float32)
        local = base + jnp.arange(local_experts, dtype=jnp.float32)
        match = ids[:, :, :, None, :] == local[None, None, None, :, None]
        member = jnp.any(match, axis=2)
        weight = jnp.sum(jnp.where(match, wts[:, :, :, None, :], 0.0), axis=2)
        upper = (jnp.arange(n_tok)[:, None] < jnp.arange(n_tok)[None, :]).astype(jnp.bfloat16)
        rank = jnp.einsum("mset,tu->mseu", member.astype(jnp.bfloat16), upper, preferred_element_type=jnp.float32)
        rank = jnp.where(member, rank, -1.0)

        residuals, blocks, shared_outs = [], [], []
        tok = tokens[0]
        for m in range(n_micro):
            residual = attention_block(tok, attn_norm, w_query, w_key, w_value, w_out).reshape(n_tok, d_model)
            normed = rms_norm(residual, ffn_norm)
            if m + 1 < n_micro:
                tok, normed = lax.optimization_barrier((tokens[m + 1], normed))
            residuals.append(residual)
            from_left = shift(normed, 1)
            from_right = shift(normed, -1)
            opp_top = shift(from_left[:half], 1)
            opp_bot = shift(from_right[half:], -1)
            blocks.append(
                {
                    "o": [opp_top, opp_bot],
                    "os": [twin(opp_top), twin(opp_bot)],
                    "l": [from_left],
                    "ls": [twin(from_left)],
                    "r": [from_right],
                    "rs": [twin(from_right)],
                    "m": [normed],
                    "ms": [twin(normed)],
                }
            )
            shared_outs.append(swiglu(normed, shared_gate, shared_up, shared_down))

        at = {"o": 0, "os": 1, "l": 2, "ls": 3, "r": 4, "rs": 5, "m": 6, "ms": 7}

        def run(m, first, second, adds=(None, None)):
            pick = lambda a: jnp.stack([a[m, at[first]], a[m, at[second]]])
            return expert_call(
                [blocks[m][first], blocks[m][second]], adds, pick(rank), pick(weight), w_gate, w_up, w_down, cap
            )

        sums = []
        for m in range(n_micro):
            opp_s, opp = run(m, "os", "o")
            opp = opp + twin(opp_s)
            got_left = shift(opp[:half], 1)
            got_right = shift(opp[half:], -1)
            right_s, left_s = run(m, "rs", "ls")
            right, left = run(m, "r", "l", (twin(right_s), twin(left_s)))
            bot_l = shift(right[half:], 1)
            top_r = shift(left[:half], -1)
            top_l = shift(right[:half] + got_left, 1)
            bot_r = shift(left[half:] + got_right, -1)
            sums.append((top_l, bot_l, top_r, bot_r))
        micro_outs = []
        for m in range(n_micro):
            own_s, own = run(m, "ms", "m")
            own_q = twin(own_s)
            top_l, bot_l, top_r, bot_r = sums[m]
            base_rows = residuals[m].astype(jnp.float32) + shared_outs[m].astype(jnp.float32)
            top = base_rows[:half] + (own[:half] + own_q[:half] + top_l + top_r)
            bot = base_rows[half:] + (own[half:] + own_q[half:] + bot_l + bot_r)
            micro_outs += [top.astype(jnp.bfloat16), bot.astype(jnp.bfloat16)]
        return jnp.stack(micro_outs).reshape(n_micro, n_seq, seq_len, d_model)

    token_spec = P(None, ("dp", "ep"), None, None)
    route_spec = P(None, ("dp", "ep"), None)
    rep_spec = P()
    expert_spec = P("ep", None, None)
    in_specs = (token_spec, route_spec, route_spec, rep_spec, rep_spec, rep_spec, rep_spec, rep_spec, rep_spec, expert_spec, expert_spec, expert_spec, rep_spec, rep_spec, rep_spec)
    return jax.shard_map(device_step, mesh=mesh, in_specs=in_specs, out_specs=token_spec, check_vma=False)
```
